32 devices in a mesh: shots: 2 (over x), mx: 16 (over z, y, core).
Axes of the slice: x: 2, y: 2, z: 4, core: 2. Of those that a mesh axis runs over, the one named last changes fastest.
Arguments:
- initial: float32 [18, 125, 2048], P('shots', None, 'mx'), parts along dimension 0, may hold values from -6 to 6
- derivative: float32 [3, 125, 125], replicated, may hold values from -0.5 to 0.5
- coupling: float32 [3, 9, 9], replicated, may hold values from -2 to 2
- face_lift: float32 [2, 125, 125], replicated, may hold values from -0.5 to 0.5
- metric: float32 [3, 2048], P(None, 'mx'), may hold values from 0.3 to 3
- rec_element: int32 [4096], P('mx'), may hold values from 0 to 127
- rec_weight: float32 [125, 4096], P(None, 'mx'), may hold values from -0.5 to 0.5
- live_counts: int32 [16], replicated, may hold values from 1 to 256, 2048 in all
- shot_order: int32 [4096], replicated, may hold values from 0 to 4095, as said below
- observed: float32 [8192, 48], P(('shots', 'mx')), parts along dimension 0, may hold values from -6 to 6
Outputs:
- residual: float32 [8192, 48], P(('shots', 'mx')), parts along dimension 0
- misfit: float32 [8192], P(('shots', 'mx')), parts along dimension 0
- adjoint: float32 [8192, 48], P(('shots', 'mx')), parts along dimension 0
The draws below stay inside these ranges and needn't reach their ends.
There are 2 independent parts, one for each index of `shots`. The reference program is written for one: setup_inputs(seed, part) draws one part's arguments, and reference() takes and returns one part's arrays. A program takes and returns all parts, laid end to end along the dimension named above; an argument that names none is the same for every part. Nothing has to cross between parts.
Inputs may be any that keep to these rules, and one draw needn't show every extreme that they name: `rec_element`: local element index of the slot within its block of 128 elements. The live receivers of block b are its first live_counts[b] slots. `shot_order`: a permutation of the slots; of the 256 positions of each block of shot-receiver order, exactly 16 come from the slots of each block.
All inputs are finite; a program needn't handle non-finite values.
Results may differ from the reference program's by a relative error of at most 0.00018.
Values sent between devices are 32-bit elements; how exact they have to be, the bound alone decides.
A program may use at most 64 MiB of HBM per device.

```python
import math
import jax
import jax.numpy as jnp
import numpy as np
from jax import lax

FIELDS = 9
NODE = 125
STEPS = 12
E_DEV = 128
R_DEV = 256
TW = 48
BLOCKS = 16
PAIR = 16
ELEMS = 2048
R_TOTAL = 4096


def draw_shot_order(key, part):
    key_a, key_b = jax.random.split(key)
    slot_perm = jax.vmap(lambda sub: jax.random.permutation(sub, R_DEV))(jax.random.split(key_a, BLOCKS))
    grouped = slot_perm.reshape(BLOCKS, BLOCKS, PAIR)
    source_ids = jnp.arange(BLOCKS, dtype=jnp.int32)[:, None, None] * R_DEV + grouped.astype(jnp.int32)
    per_dest = source_ids.transpose(1, 0, 2).reshape(BLOCKS, R_DEV)
    dest_order = jax.vmap(lambda sub: jax.random.permutation(sub, R_DEV))(jax.random.split(key_b, BLOCKS))
    placed = jnp.take_along_axis(per_dest, dest_order.astype(jnp.int32), axis=1)
    return placed.reshape(-1).astype(jnp.int32)


def with_ends(drawn, rng, least, largest):
    longest = drawn.shape.index(max(drawn.shape))
    spots = []
    for shift in (0, 1):
        where = [jax.random.randint(jax.random.fold_in(rng, axis), (), 0, length) for axis, length in enumerate(drawn.shape)]
        where[longest] = (where[longest] + shift) % drawn.shape[longest]
        spots.append(tuple(where))
    return drawn.at[spots[0]].set(least).at[spots[1]].set(largest)


def level_of(key, extent, pieces, low, high):
    loudness = 1.0
    for position, shards_of in pieces:
        heights = jax.random.uniform(jax.random.fold_in(jax.random.fold_in(key, 6), position), (shards_of,), jnp.float32, low / len(pieces), high / len(pieces))
        loudness = loudness * jnp.repeat(jnp.exp(heights), extent[position] // shards_of).reshape((-1,) + (1,) * (len(extent) - 1 - position))
    return loudness


def split_up(count, total, most, slope):
    loads = [(1 << 20) // math.isqrt(standing ** slope) + 1 for standing in range(2, count + 1)]
    spare, counts = total - most - (count - 1), [1] * (count - 1)
    while spare > 0:
        free = [i for i in range(count - 1) if counts[i] < most]
        pool, left = sum([loads[i] for i in free]), spare
        for i in free:
            extra = min(most - counts[i], max(1, left * loads[i] // pool), spare)
            counts[i] = counts[i] + extra
            spare = spare - extra
    return np.array([most] + counts)


def ragged_sizes(stream_key, number_of, total, limit, lean):
    if number_of == 2:
        one = jax.random.randint(stream_key, (), max(1, total - limit), min(limit, total - 1) + 1)
        return jnp.stack([one, total - one])
    tallies = jnp.asarray(split_up(number_of, total, limit, lean), jnp.int32)
    pairs = (number_of - 1) // 2
    donor, receiver = tallies[1:1 + 2 * pairs:2], tallies[2:2 + 2 * pairs:2]
    margin = jnp.minimum(donor - 1, limit - receiver)
    passed = jax.random.randint(jax.random.fold_in(stream_key, 1), (pairs,), 0, 1 << 20) % (margin + 1)
    tallies = tallies.at[1:1 + 2 * pairs:2].set(donor - passed).at[2:2 + 2 * pairs:2].set(receiver + passed)
    return tallies[jax.random.permutation(jax.random.fold_in(stream_key, 2), number_of)]


def normal_values(own_key, extent, spread, most, pieces=(), kind=jnp.bfloat16):
    result = spread * jax.random.normal(own_key, extent, jnp.float32)
    if pieces:
        result = result * level_of(own_key, extent, pieces, -0.22, 0.18)
    return jnp.clip(result, -most, most).astype(kind)


def setup_inputs(seed: int = 0, part: int = 0) -> dict:
    key_list = jax.random.split(jax.random.key(seed), 11)
    part_splits = jax.random.split(jax.random.fold_in(key_list[10], part), 11)
    initial = normal_values(part_splits[0], (FIELDS, NODE, ELEMS), 1.0, 6.0, ((2, 16),), jnp.float32)
    derivative = normal_values(key_list[1], (3, NODE, NODE), NODE ** -0.5, 0.5, (), jnp.float32)
    coupling = normal_values(key_list[2], (3, FIELDS, FIELDS), FIELDS ** -0.5, 2.0, (), jnp.float32)
    face_lift = normal_values(key_list[3], (2, NODE, NODE), NODE ** -0.5, 0.5, (), jnp.float32)
    metric = jnp.clip(jnp.exp(math.log(3.0) - 2.3025851 * jax.random.uniform(key_list[4], (3, ELEMS), jnp.float32) ** level_of(key_list[4], (3, ELEMS), ((1, 16),), -0.2, 0.2)), 0.3, 3.0)
    rec_element = with_ends(jax.random.randint(key_list[5], (R_TOTAL,), 0, E_DEV), jax.random.fold_in(key_list[5], 1), 0, E_DEV - 1).astype(jnp.int32)
    rec_weight = normal_values(key_list[6], (NODE, R_TOTAL), NODE ** -0.5, 0.5, ((1, 16),), jnp.float32)
    live_counts = ragged_sizes(key_list[7], BLOCKS, BLOCKS * R_DEV // 2, R_DEV, 2).astype(jnp.int32)
    shot_order = draw_shot_order(jax.random.fold_in(key_list[10], 71), part)
    observed = normal_values(part_splits[9], (R_TOTAL, TW), 1.0, 6.0, ((0, 16),), jnp.float32)
    return dict(initial=initial, derivative=derivative, coupling=coupling, face_lift=face_lift, metric=metric, rec_element=rec_element, rec_weight=rec_weight, live_counts=live_counts, shot_order=shot_order, observed=observed)


HIGH = lax.Precision.HIGHEST


def advance(extended, metric_cols, derivative, coupling, face_lift, time_step):
    middle = extended[:, :, 1:-1]
    summed = jnp.einsum('pq,fqe->fpe', face_lift[0], extended[:, :, :-2] - middle, precision=HIGH)
    summed = summed + jnp.einsum('pq,fqe->fpe', face_lift[1], extended[:, :, 2:] - middle, precision=HIGH)
    for k in range(3):
        gradient = jnp.einsum('pq,fqe->fpe', derivative[k], middle, precision=HIGH)
        summed = summed + jnp.einsum('gf,fpe->gpe', coupling[k], gradient, precision=HIGH) * metric_cols[k][None, None, :]
    return middle + time_step * summed


def sample(wavefield, elements, rec_weight, live_slot):
    components = jnp.stack([wavefield[0], wavefield[1], wavefield[2], (wavefield[3] + wavefield[4] + wavefield[5]) / 3.0])
    columns = jnp.take(components, elements, axis=2)
    return jnp.sum(columns * rec_weight[None], axis=1) * live_slot[None]


def reference(initial, derivative, coupling, face_lift, metric, rec_element, rec_weight, live_counts, shot_order, observed):
    time_step = 0.5 / STEPS
    slot_ids = jnp.arange(R_TOTAL, dtype=jnp.int32)
    block_of = slot_ids // R_DEV
    global_elem = (block_of * E_DEV + rec_element).astype(jnp.int32)
    live_slot = ((slot_ids % R_DEV) < live_counts[block_of]).astype(jnp.float32)

    def one_step(t, carry):
        wavefield, trace_buffer = carry
        extended = jnp.pad(wavefield, ((0, 0), (0, 0), (1, 1)))
        wavefield = advance(extended, metric, derivative, coupling, face_lift, time_step)
        sampled = sample(wavefield, global_elem, rec_weight, live_slot)
        trace_buffer = lax.dynamic_update_slice(trace_buffer, sampled[:, None, :], (0, t, 0))
        return wavefield, trace_buffer

    trace_buffer = jnp.zeros((4, STEPS, R_TOTAL), jnp.float32)
    final_field, trace_buffer = lax.fori_loop(0, STEPS, one_step, (initial, trace_buffer))
    synthetic = trace_buffer.transpose(2, 0, 1).reshape(R_TOTAL, 4 * STEPS)
    ordered = synthetic[shot_order]
    live_out = live_slot[shot_order]
    residual = live_out[:, None] * (ordered - observed)
    misfit = 0.5 * jnp.sum(residual * residual, axis=1)
    flipped = residual.reshape(R_TOTAL, 4, STEPS)[:, :, ::-1].reshape(R_TOTAL, 4 * STEPS)
    adjoint = jnp.zeros_like(flipped).at[shot_order].set(flipped)
    return residual, misfit, adjoint
```

```python
import functools
import jax
import jax.numpy as jnp
from jax import lax
from jax.experimental import pallas as pl
from jax.experimental.pallas import tpu as pltpu
from jax.sharding import PartitionSpec as P

STEPS = 12
COMPS = 4
HALO = 16
GUARD = 8
HIGH = lax.Precision.HIGHEST


def split(x):
    hi = x.astype(jnp.bfloat16)
    return hi, (x - hi.astype(jnp.float32)).astype(jnp.bfloat16)


def wave_kernel(own, low, high, metric, mask, wmat, weight, elem, live, cpl, out, ubuf, lhs, wb, ws, hist):
    fields, count, lanes = own.shape
    first = GUARD + HALO
    kdim = wmat.shape[0]
    rows_all = ubuf.shape[2]
    for b in range(2):
        for f in range(fields):
            ubuf[b, f] = jnp.zeros((rows_all, lanes), jnp.float32)
    for f in range(fields):
        ubuf[0, f, GUARD:first] = low[f]
        ubuf[0, f, first:first + count] = own[f]
        ubuf[0, f, first + count:first + count + HALO] = high[f]
    for k in range(kdim // lanes):
        hi, lo = split(wmat[k * lanes:(k + 1) * lanes])
        for base in (0, kdim):
            wb[base + k * lanes:base + (k + 1) * lanes, :lanes] = hi
            wb[base + k * lanes:base + (k + 1) * lanes, lanes:] = lo
    hi, lo = split(weight[...])
    ws[0:lanes] = hi
    ws[lanes:2 * lanes] = hi
    ws[2 * lanes:] = lo

    def mix(src, c, halo, slab):
        rows = count + 2 * halo
        base = first - halo
        for gi in range(3):
            g = c * 3 + gi
            for r in range(0, rows, slab):
                acc = [None] * 3
                for f in range(fields):
                    uf = ubuf[src, f, base + r:base + r + slab]
                    for k in range(3):
                        term = cpl[(k * fields + g) * fields + f] * uf
                        acc[k] = term if acc[k] is None else acc[k] + term
                at = gi * rows + r
                mid = ubuf[src, g, base + r:base + r + slab]
                vals = [acc[k] * metric[k, HALO - halo + r:HALO - halo + r + slab] for k in range(3)]
                vals.append(ubuf[src, g, base + r - 1:base + r - 1 + slab] - mid)
                vals.append(ubuf[src, g, base + r + 1:base + r + 1 + slab] - mid)
                for k, v in enumerate(vals):
                    hi, lo = split(v)
                    lhs[c, at:at + slab, k * lanes:(k + 1) * lanes] = hi
                    lhs[c, at:at + slab, kdim + k * lanes:kdim + (k + 1) * lanes] = lo

    def apply(src, dst, c, halo):
        rows = count + 2 * halo
        base = first - halo
        res = jnp.dot(lhs[c, :3 * rows], wb[...], preferred_element_type=jnp.float32)
        for gi in range(3):
            g = c * 3 + gi
            part = res[gi * rows:(gi + 1) * rows]
            new = ubuf[src, g, base:base + rows] + (part[:, :lanes] + part[:, lanes:])
            ubuf[dst, g, base:base + rows] = new * mask[HALO - halo:HALO - halo + rows]

    def step(halo, slab, t, _):
        src = lax.rem(t, 2)
        dst = 1 - src
        mix(src, 0, halo, slab)
        mix(src, 1, halo, slab)
        apply(src, dst, 0, halo)
        mix(src, 2, halo, slab)
        apply(src, dst, 1, halo)
        apply(src, dst, 2, halo)
        mine = slice(first, first + count)
        vals = [ubuf[dst, c, mine] for c in range(3)]
        vals.append((ubuf[dst, 3, mine] + ubuf[dst, 4, mine] + ubuf[dst, 5, mine]) / 3.0)
        for c, v in enumerate(vals):
            hi, lo = split(v)
            hist[t, c, :, 0:lanes] = hi
            hist[t, c, :, lanes:2 * lanes] = lo
            hist[t, c, :, 2 * lanes:] = hi
        return 0

    lax.fori_loop(0, 3, functools.partial(step, 16, 80), 0)
    lax.fori_loop(3, STEPS, functools.partial(step, 8, 48), 0)

    slots = weight.shape[1]
    ids = lax.broadcasted_iota(jnp.int32, (count, slots), 0)
    pick = jnp.where(ids == elem[...], live[...], 0.0)

    def sample(t, _):
        for c in range(COMPS):
            prod = jnp.dot(hist[t, c], ws[...], preferred_element_type=jnp.float32)
            out[pl.ds(c * STEPS + t, 1), :] = jnp.sum(prod * pick, axis=0, keepdims=True)
        return 0

    lax.fori_loop(0, STEPS, sample, 0)


def waves(own, low, high, metric, mask, wmat, weight, elem, live, cpl):
    fields, count, lanes = own.shape
    slots = weight.shape[1]
    vm = pl.BlockSpec(memory_space=pltpu.VMEM)
    return pl.pallas_call(
        wave_kernel,
        out_shape=jax.ShapeDtypeStruct((COMPS * STEPS, slots), jnp.float32),
        in_specs=[vm] * 9 + [pl.BlockSpec(memory_space=pltpu.SMEM)],
        out_specs=vm,
        scratch_shapes=[
            pltpu.VMEM((2, fields, count + 2 * (HALO + GUARD), lanes), jnp.float32),
            pltpu.VMEM((3, 3 * (count + 2 * HALO), 2 * wmat.shape[0]), jnp.bfloat16),
            pltpu.VMEM((2 * wmat.shape[0], 2 * lanes), jnp.bfloat16),
            pltpu.VMEM((3 * lanes, slots), jnp.bfloat16),
            pltpu.VMEM((STEPS, COMPS, count, 3 * lanes), jnp.bfloat16),
        ],
        cost_estimate=pl.CostEstimate(flops=10**10, bytes_accessed=2 * 10**6, transcendentals=0),
        name="waves",
    )(own, low, high, metric, mask, wmat, weight, elem, live, cpl)


def flip(rows):
    return rows.reshape(-1, COMPS, STEPS)[:, :, ::-1].reshape(-1, COMPS * STEPS)


def shards(initial, derivative, coupling, face_lift, metric, rec_element, rec_weight, live_counts, shot_order, observed):
    time_step = 0.5 / STEPS
    fields, nodes, elems = initial.shape
    lanes = -(-nodes // 128) * 128
    slots = rec_element.shape[0]
    peers = lax.axis_size("mx")
    pair = slots // peers
    me = lax.axis_index("mx")
    up = [(i, i + 1) for i in range(peers - 1)]
    down = [(b, a) for a, b in up]
    pad = lanes - nodes

    own = jnp.pad(initial.transpose(0, 2, 1), ((0, 0), (0, 0), (0, pad)))
    met = metric.T
    low = lax.ppermute(own[:, elems - HALO:], "mx", up)
    high = lax.ppermute(own[:, :HALO], "mx", down)
    met_low = lax.ppermute(met[elems - HALO:], "mx", up)
    met_high = lax.ppermute(met[:HALO], "mx", down)
    met_all = jnp.concatenate([met_low, met, met_high], axis=0).T
    met_wide = jnp.broadcast_to(met_all[:, :, None], met_all.shape + (lanes,))
    ids = me * elems - HALO + jnp.arange(elems + 2 * HALO, dtype=jnp.int32)
    inside = ((ids >= 0) & (ids < elems * peers)).astype(jnp.float32)
    inside = jnp.broadcast_to(inside[:, None], (elems + 2 * HALO, lanes))
    mats = jnp.concatenate([derivative, face_lift], axis=0).transpose(0, 2, 1) * time_step
    wmat = jnp.pad(mats, ((0, 0), (0, pad), (0, pad))).reshape(-1, lanes)
    weight = jnp.pad(rec_weight, ((0, pad), (0, 0)))

    slot_ids = jnp.arange(slots, dtype=jnp.int32)
    live = (slot_ids < live_counts[me]).astype(jnp.float32)
    by_block = shot_order.reshape(peers, slots)
    source, slot = by_block // slots, by_block % slots
    tri = (slot_ids[:, None] <= slot_ids[None, :]).astype(jnp.float32)
    mine = source == me
    rank = jnp.dot(mine.astype(jnp.float32), tri).astype(jnp.int32) - 1
    hit = mine[:, None, :] & (rank[:, None, :] == jnp.arange(pair, dtype=jnp.int32)[None, :, None])
    send_slot = jnp.sum(jnp.where(hit, slot[:, None, :], 0), axis=2).reshape(-1)
    to_send = (send_slot[:, None] == slot_ids[None, :]).astype(jnp.float32)
    own_source = lax.dynamic_index_in_dim(source, me, 0, keepdims=False)
    own_slot = lax.dynamic_index_in_dim(slot, me, 0, keepdims=False)
    from_peer = own_source[None, :] == jnp.arange(peers, dtype=jnp.int32)[:, None]
    count = jnp.dot(from_peer.astype(jnp.float32), tri).astype(jnp.int32) - 1
    own_rank = jnp.sum(jnp.where(from_peer, count, 0), axis=0)
    place = own_source * pair + own_rank
    to_place = (place[:, None] == slot_ids[None, :]).astype(jnp.float32)
    own_counts = jnp.sum(jnp.where(from_peer, live_counts[:, None], 0), axis=0)
    live_out = (own_slot < own_counts).astype(jnp.float32)

    def exchange(rows):
        moved = lax.all_to_all(rows.reshape(peers, pair, -1), "mx", split_axis=0, concat_axis=0, tiled=True)
        return moved.reshape(slots, -1)

    sorted_obs = jnp.dot(to_place.T, observed, precision=HIGH)
    slot_obs = jnp.dot(to_send.T, exchange(sorted_obs), precision=HIGH)

    traces = waves(own, low, high, met_wide, inside, wmat, weight, rec_element[None, :], live[None, :], coupling.reshape(-1))
    synthetic = traces.T
    packed = lax.dot_general(to_send, traces, (((1,), (1,)), ((), ())), precision=HIGH)
    ordered = jnp.dot(to_place, exchange(packed), precision=HIGH)
    residual = live_out[:, None] * (ordered - observed)
    misfit = 0.5 * jnp.sum(residual * residual, axis=1)
    adjoint = live[:, None] * flip(synthetic - slot_obs)
    return residual, misfit, adjoint


def solution(mesh):
    in_specs = (
        P("shots", None, "mx"),
        P(),
        P(),
        P(),
        P(None, "mx"),
        P("mx"),
        P(None, "mx"),
        P(),
        P(),
        P(("shots", "mx"), None),
    )
    out_specs = (P(("shots", "mx"), None), P(("shots", "mx")), P(("shots", "mx"), None))
    return jax.shard_map(shards, mesh=mesh, in_specs=in_specs, out_specs=out_specs, check_vma=False)
```

```python
import functools
import jax
import jax.numpy as jnp
from jax import lax
from jax.experimental import pallas as pl
from jax.experimental.pallas import tpu as pltpu
from jax.sharding import PartitionSpec as P

STEPS = 12
COMPS = 4
HALO = 16
GUARD = 8


def split(x):
    hi = x.astype(jnp.bfloat16)
    return hi, (x - hi.astype(jnp.float32)).astype(jnp.bfloat16)


def zeros(*shape):
    return jnp.zeros(shape, jnp.float32)


def ones_where(cond):
    return jnp.where(cond, 1.0, 0.0).astype(jnp.bfloat16)


def dot(a, b):
    return jnp.dot(a, b, preferred_element_type=jnp.float32)


def permute(onehot, x):
    hi = x.astype(jnp.bfloat16)
    rest = x - hi.astype(jnp.float32)
    mid = rest.astype(jnp.bfloat16)
    low = (rest - mid.astype(jnp.float32)).astype(jnp.bfloat16)
    return dot(onehot, hi) + (dot(onehot, mid) + dot(onehot, low))


def greet(peers, me):
    barrier = pltpu.get_barrier_semaphore()

    def one(off, _):
        pl.semaphore_signal(barrier, inc=1, device_id={"mx": lax.rem(me + off, peers)}, device_id_type=pl.DeviceIdType.MESH)
        return 0

    lax.fori_loop(1, peers, one, 0)
    return barrier


def start_kernel(peers, initial, metric, mats, weight_in, order, counts,
                 state, wb, ws, to_send, from_send, to_place, from_place, live,
                 pad, padw, send_sem, recv_sem):
    fields, nodes, count = initial.shape
    lanes = pad.shape[0]
    slots = order.shape[1]
    pair = slots // peers
    me = lax.axis_index("mx")
    right, left = lax.rem(me + 1, peers), lax.rem(me + peers - 1, peers)
    barrier = pltpu.get_barrier_semaphore()
    for side in (left, right):
        pl.semaphore_signal(barrier, inc=1, device_id={"mx": side}, device_id_type=pl.DeviceIdType.MESH)
    pad[...] = zeros(lanes, lanes)
    for f in range(fields):
        pad[0:nodes, :] = initial[f]
        state[f, HALO:HALO + count] = pad[...].T
    kinds = metric.shape[0]
    for k in range(kinds):
        state[fields + k, HALO:HALO + count] = jnp.broadcast_to(metric[k:k + 1, :], (lanes, count)).T
    pl.semaphore_wait(barrier, 2)
    moved = fields + kinds
    copies = []
    for i, (side, at, to) in enumerate(((right, count, 0), (left, HALO, HALO + count))):
        copies.append(pltpu.make_async_remote_copy(
            src_ref=state.at[0:moved, at:at + HALO], dst_ref=state.at[0:moved, to:to + HALO],
            send_sem=send_sem.at[i], recv_sem=recv_sem.at[i],
            device_id={"mx": side}, device_id_type=pl.DeviceIdType.MESH))
        copies[-1].start()
    pad[...] = zeros(lanes, lanes)
    kdim = mats.shape[0] * lanes
    for k in range(mats.shape[0]):
        pad[0:nodes, 0:nodes] = mats[k]
        hi, lo = split(pad[...].T * (0.5 / STEPS))
        for base in (0, kdim):
            wb[base + k * lanes:base + (k + 1) * lanes, :lanes] = hi
            wb[base + k * lanes:base + (k + 1) * lanes, lanes:] = lo
    padw[...] = zeros(lanes, slots)
    padw[0:nodes, :] = weight_in[...]
    hi, lo = split(padw[...])
    ws[0:lanes] = hi
    ws[lanes:2 * lanes] = hi
    ws[2 * lanes:] = lo
    rows = lax.broadcasted_iota(jnp.int32, (count + 2 * HALO, lanes), 0) + (me * count - HALO)
    state[moved] = jnp.where((rows >= 0) & (rows < count * peers), 1.0, 0.0)

    up = lax.broadcasted_iota(jnp.int32, (slots, slots), 0)
    across = lax.broadcasted_iota(jnp.int32, (slots, slots), 1)
    tri = ones_where(up <= across)
    blocks = order[...]
    source, slot = lax.div(blocks, slots), lax.rem(blocks, slots)
    mine = source == me
    rank = dot(ones_where(mine), tri) - 1.0
    rank = jnp.where(mine, rank, -1.0)
    tall = lax.broadcasted_iota(jnp.int32, (slots, peers), 0)
    wide = lax.broadcasted_iota(jnp.int32, (slots, peers), 1)
    repeat = ones_where(lax.div(tall, pair) == wide)
    rank_all = dot(repeat, rank.astype(jnp.bfloat16))
    slot_all = dot(repeat, slot.astype(jnp.float32).astype(jnp.bfloat16))
    hit = rank_all == lax.rem(up, pair).astype(jnp.float32)
    send_slot = jnp.sum(jnp.where(hit, slot_all, 0.0), axis=1, keepdims=True)
    sends = jnp.where(send_slot == across.astype(jnp.float32), 1.0, 0.0)
    to_send[...] = sends.astype(jnp.bfloat16)
    from_send[...] = sends.T.astype(jnp.bfloat16)
    own = order[pl.ds(me, 1), :]
    own_source = lax.div(own, slots)
    peer_ids = lax.broadcasted_iota(jnp.int32, (peers, slots), 0)
    from_peer = peer_ids == own_source
    seen = dot(ones_where(from_peer), tri) - 1.0
    own_rank = jnp.sum(jnp.where(from_peer, seen, 0.0), axis=0, keepdims=True)
    place = own_source.astype(jnp.float32) * float(pair) + own_rank
    places = jnp.where(up.astype(jnp.float32) == place, 1.0, 0.0)
    to_place[...] = places.astype(jnp.bfloat16)
    from_place[...] = places.T.astype(jnp.bfloat16)
    limit = counts[pl.ds(me, 1), :]
    live[...] = jnp.where(lax.broadcasted_iota(jnp.int32, (1, slots), 1) < limit, 1.0, 0.0)
    for copy in copies:
        copy.wait()


def end_kernel(peers, traces, observed, to_send, from_send, to_place, from_place,
               residual, misfit, adjoint, sent, got, send_sem, recv_sem):
    slots, width = observed.shape
    lanes = sent.shape[-1]
    wide = traces.shape[0]
    pair = slots // peers
    me = lax.axis_index("mx")
    barrier = greet(peers, me)
    synth = traces[...].T
    packed = permute(to_send[...], synth)
    obs = permute(to_place[...], observed[...])
    row = jnp.concatenate([packed, obs, zeros(slots, lanes - wide - width)], axis=1)
    sent[...] = row.reshape(peers, pair, lanes)
    pl.semaphore_wait(barrier, peers - 1)

    def copy_to(off):
        dest = lax.rem(me + off, peers)
        return pltpu.make_async_remote_copy(
            src_ref=sent.at[dest], dst_ref=got.at[me], send_sem=send_sem.at[dest], recv_sem=recv_sem.at[me],
            device_id={"mx": dest}, device_id_type=pl.DeviceIdType.MESH)

    def copy_from(off):
        src = lax.rem(me - off + peers, peers)
        return pltpu.make_async_remote_copy(
            src_ref=sent.at[src], dst_ref=got.at[src], send_sem=send_sem.at[src], recv_sem=recv_sem.at[src],
            device_id={"mx": src}, device_id_type=pl.DeviceIdType.MESH)

    def begin(off, _):
        copy_to(off).start()
        return 0

    def finish(off, _):
        copy_from(off).wait_recv()
        return 0

    def drain(off, _):
        copy_to(off).wait_send()
        return 0

    lax.fori_loop(1, peers, begin, 0)
    got[pl.ds(me, 1)] = sent[pl.ds(me, 1)]
    lax.fori_loop(1, peers, finish, 0)
    arrived = got[...].reshape(slots, lanes)
    placed = permute(from_place[...], arrived[:, :wide])
    res = placed[:, width:width + 1] * (placed[:, :width] - observed[...])
    residual[...] = res
    misfit[...] = 0.5 * jnp.sum(res * res, axis=1, keepdims=True)
    slot_obs = permute(from_send[...], arrived[:, wide:wide + width])
    plain = synth[:, width:width + 1] * (synth[:, :width] - slot_obs)
    a = lax.broadcasted_iota(jnp.int32, (width, width), 0)
    b = lax.broadcasted_iota(jnp.int32, (width, width), 1)
    back = ones_where((lax.div(a, STEPS) == lax.div(b, STEPS)) & (lax.rem(a, STEPS) + lax.rem(b, STEPS) == STEPS - 1))
    hi = plain.astype(jnp.bfloat16)
    rest = plain - hi.astype(jnp.float32)
    mid = rest.astype(jnp.bfloat16)
    low = (rest - mid.astype(jnp.float32)).astype(jnp.bfloat16)
    adjoint[...] = dot(hi, back) + (dot(mid, back) + dot(low, back))
    lax.fori_loop(1, peers, drain, 0)


def wave_kernel(state, wb, ws, elem, live, cpl, out, ubuf, lhs, hist):
    fields = ubuf.shape[1]
    lanes = state.shape[2]
    count = state.shape[1] - 2 * HALO
    first = GUARD + HALO
    kdim = wb.shape[0] // 2
    rows_all = ubuf.shape[2]
    metric = state.at[fields:fields + 3]
    mask = state.at[fields + 3]
    for b in range(2):
        for f in range(fields):
            ubuf[b, f, 0:GUARD] = zeros(GUARD, lanes)
            ubuf[b, f, rows_all - GUARD:] = zeros(GUARD, lanes)
            if b:
                ubuf[b, f] = zeros(rows_all, lanes)
            else:
                ubuf[b, f, GUARD:rows_all - GUARD] = state[f] * mask[...]

    def mix(src, c, halo, slab):
        rows = count + 2 * halo
        base = first - halo
        for gi in range(3):
            g = c * 3 + gi
            for r in range(0, rows, slab):
                acc = [None] * 3
                for f in range(fields):
                    uf = ubuf[src, f, base + r:base + r + slab]
                    for k in range(3):
                        term = cpl[(k * fields + g) * fields + f] * uf
                        acc[k] = term if acc[k] is None else acc[k] + term
                at = gi * rows + r
                mid = ubuf[src, g, base + r:base + r + slab]
                vals = [acc[k] * metric[k, HALO - halo + r:HALO - halo + r + slab] for k in range(3)]
                vals.append(ubuf[src, g, base + r - 1:base + r - 1 + slab] - mid)
                vals.append(ubuf[src, g, base + r + 1:base + r + 1 + slab] - mid)
                for k, v in enumerate(vals):
                    hi, lo = split(v)
                    lhs[c, at:at + slab, k * lanes:(k + 1) * lanes] = hi
                    lhs[c, at:at + slab, kdim + k * lanes:kdim + (k + 1) * lanes] = lo

    def apply(src, dst, c, halo):
        rows = count + 2 * halo
        base = first - halo
        res = jnp.dot(lhs[c, :3 * rows], wb[...], preferred_element_type=jnp.float32)
        for gi in range(3):
            g = c * 3 + gi
            part = res[gi * rows:(gi + 1) * rows]
            new = ubuf[src, g, base:base + rows] + (part[:, :lanes] + part[:, lanes:])
            ubuf[dst, g, base:base + rows] = new * mask[HALO - halo:HALO - halo + rows]

    def step(halo, slab, t, _):
        src = lax.rem(t, 2)
        dst = 1 - src
        mix(src, 0, halo, slab)
        mix(src, 1, halo, slab)
        apply(src, dst, 0, halo)
        mix(src, 2, halo, slab)
        apply(src, dst, 1, halo)
        apply(src, dst, 2, halo)
        mine = slice(first, first + count)
        vals = [ubuf[dst, c, mine] for c in range(3)]
        vals.append((ubuf[dst, 3, mine] + ubuf[dst, 4, mine] + ubuf[dst, 5, mine]) / 3.0)
        for c, v in enumerate(vals):
            hi, lo = split(v)
            hist[t, c, :, 0:lanes] = hi
            hist[t, c, :, lanes:2 * lanes] = lo
            hist[t, c, :, 2 * lanes:] = hi
        return 0

    lax.fori_loop(0, 3, functools.partial(step, 16, 80), 0)
    lax.fori_loop(3, STEPS, functools.partial(step, 8, 48), 0)

    slots = ws.shape[1]
    ids = lax.broadcasted_iota(jnp.int32, (count, slots), 0)
    pick = jnp.where(ids == elem[...], live[...], 0.0)

    out[...] = zeros(*out.shape)
    out[COMPS * STEPS:COMPS * STEPS + 1, :] = live[...]

    def sample(t, _):
        for c in range(COMPS):
            prod = jnp.dot(hist[t, c], ws[...], preferred_element_type=jnp.float32)
            out[pl.ds(c * STEPS + t, 1), :] = jnp.sum(prod * pick, axis=0, keepdims=True)
        return 0

    lax.fori_loop(0, STEPS, sample, 0)


VM = pl.BlockSpec(memory_space=pltpu.VMEM)


def shards(initial, derivative, coupling, face_lift, metric, rec_element, rec_weight, live_counts, shot_order, observed):
    fields, nodes, count = initial.shape
    lanes = -(-nodes // 128) * 128
    slots, width = observed.shape
    peers = lax.axis_size("mx")
    mats = jnp.concatenate([derivative, face_lift], axis=0)
    span = count + 2 * HALO
    kdim = mats.shape[0] * lanes
    wide = -(-(width + 1) // 64) * 64
    f32, bf16 = jnp.float32, jnp.bfloat16
    square = jax.ShapeDtypeStruct((slots, slots), bf16)
    state, wb, ws, to_send, from_send, to_place, from_place, live = pl.pallas_call(
        functools.partial(start_kernel, peers),
        out_shape=(
            jax.ShapeDtypeStruct((fields + metric.shape[0] + 1, span, lanes), f32),
            jax.ShapeDtypeStruct((2 * kdim, 2 * lanes), bf16),
            jax.ShapeDtypeStruct((3 * lanes, slots), bf16),
            square, square, square, square,
            jax.ShapeDtypeStruct((1, slots), f32),
        ),
        in_specs=[VM] * 6,
        out_specs=[VM] * 8,
        scratch_shapes=[
            pltpu.VMEM((lanes, lanes), f32),
            pltpu.VMEM((lanes, slots), f32),
            pltpu.SemaphoreType.DMA((2,)),
            pltpu.SemaphoreType.DMA((2,)),
        ],
        compiler_params=pltpu.CompilerParams(collective_id=0, has_side_effects=True),
        name="start",
    )(initial, metric, mats, rec_weight, shot_order.reshape(peers, slots), live_counts[:, None])
    traces = pl.pallas_call(
        wave_kernel,
        out_shape=jax.ShapeDtypeStruct((wide, slots), f32),
        in_specs=[VM] * 5 + [pl.BlockSpec(memory_space=pltpu.SMEM)],
        out_specs=VM,
        scratch_shapes=[
            pltpu.VMEM((2, fields, span + 2 * GUARD, lanes), f32),
            pltpu.VMEM((3, 3 * span, 2 * kdim), bf16),
            pltpu.VMEM((STEPS, COMPS, count, 3 * lanes), bf16),
        ],
        name="waves",
    )(state, wb, ws, rec_element[None, :], live, coupling.reshape(-1))
    residual, misfit, adjoint = pl.pallas_call(
        functools.partial(end_kernel, peers),
        out_shape=(
            jax.ShapeDtypeStruct((slots, width), f32),
            jax.ShapeDtypeStruct((slots, 1), f32),
            jax.ShapeDtypeStruct((slots, width), f32),
        ),
        in_specs=[VM] * 6,
        out_specs=[VM] * 3,
        scratch_shapes=[
            pltpu.VMEM((peers, slots // peers, lanes), f32),
            pltpu.VMEM((peers, slots // peers, lanes), f32),
            pltpu.SemaphoreType.DMA((peers,)),
            pltpu.SemaphoreType.DMA((peers,)),
        ],
        compiler_params=pltpu.CompilerParams(collective_id=1, has_side_effects=True),
        name="finish",
    )(traces, observed, to_send, from_send, to_place, from_place)
    return residual, misfit[:, 0], adjoint


def solution(mesh):
    in_specs = (
        P("shots", None, "mx"),
        P(),
        P(),
        P(),
        P(None, "mx"),
        P("mx"),
        P(None, "mx"),
        P(),
        P(),
        P(("shots", "mx"), None),
    )
    out_specs = (P(("shots", "mx"), None), P(("shots", "mx")), P(("shots", "mx"), None))
    return jax.shard_map(shards, mesh=mesh, in_specs=in_specs, out_specs=out_specs, check_vma=False)
```

```python
import functools
import jax
import jax.numpy as jnp
from jax import lax
from jax.experimental import pallas as pl
from jax.experimental.pallas import tpu as pltpu
from jax.sharding import PartitionSpec as P

STEPS = 12
COMPS = 4
HALO = 16
GUARD = 8


def split(x):
    hi = x.astype(jnp.bfloat16)
    return hi, (x - hi.astype(jnp.float32)).astype(jnp.bfloat16)


def zeros(*shape):
    return jnp.zeros(shape, jnp.float32)


def ones_where(cond):
    return jnp.where(cond, 1.0, 0.0).astype(jnp.bfloat16)


def dot(a, b):
    return jnp.dot(a, b, preferred_element_type=jnp.float32)


def permute(onehot, x):
    hi = x.astype(jnp.bfloat16)
    rest = x - hi.astype(jnp.float32)
    mid = rest.astype(jnp.bfloat16)
    low = (rest - mid.astype(jnp.float32)).astype(jnp.bfloat16)
    return dot(onehot, hi) + (dot(onehot, mid) + dot(onehot, low))


def greet(peers, me):
    barrier = pltpu.get_barrier_semaphore()

    def one(off, _):
        pl.semaphore_signal(barrier, inc=1, device_id={"mx": lax.rem(me + off, peers)}, device_id_type=pl.DeviceIdType.MESH)
        return 0

    lax.fori_loop(1, peers, one, 0)
    return barrier


def start_kernel(peers, initial, metric, derivative, face_lift, weight_in, order, counts,
                 state, wb, ws, to_send, from_send, to_place, from_place, live,
                 pad, padw, send_sem, recv_sem):
    fields, nodes, count = initial.shape
    lanes = pad.shape[0]
    slots = order.shape[1]
    pair = slots // peers
    me = lax.axis_index("mx")
    right, left = lax.rem(me + 1, peers), lax.rem(me + peers - 1, peers)
    barrier = pltpu.get_barrier_semaphore()
    for side in (left, right):
        pl.semaphore_signal(barrier, inc=1, device_id={"mx": side}, device_id_type=pl.DeviceIdType.MESH)
    pad[...] = zeros(lanes, lanes)
    for f in range(fields):
        pad[0:nodes, :] = initial[f]
        state[f, HALO:HALO + count] = pad[...].T
    kinds = metric.shape[0]
    for k in range(kinds):
        state[fields + k, HALO:HALO + count] = jnp.broadcast_to(metric[k:k + 1, :], (lanes, count)).T
    pl.semaphore_wait(barrier, 2)
    moved = fields + kinds
    copies = []
    for i, (side, at, to) in enumerate(((right, count, 0), (left, HALO, HALO + count))):
        copies.append(pltpu.make_async_remote_copy(
            src_ref=state.at[0:moved, at:at + HALO], dst_ref=state.at[0:moved, to:to + HALO],
            send_sem=send_sem.at[i], recv_sem=recv_sem.at[i],
            device_id={"mx": side}, device_id_type=pl.DeviceIdType.MESH))
        copies[-1].start()
    pad[...] = zeros(lanes, lanes)
    turns = derivative.shape[0]
    kdim = (turns + face_lift.shape[0]) * lanes
    for k in range(kdim // lanes):
        pad[0:nodes, 0:nodes] = derivative[k] if k < turns else face_lift[k - turns]
        hi, lo = split(pad[...].T * (0.5 / STEPS))
        for base in (0, kdim):
            wb[base + k * lanes:base + (k + 1) * lanes, :lanes] = hi
            wb[base + k * lanes:base + (k + 1) * lanes, lanes:] = lo
    padw[...] = zeros(lanes, slots)
    padw[0:nodes, :] = weight_in[...]
    hi, lo = split(padw[...])
    ws[0:lanes] = hi
    ws[lanes:2 * lanes] = hi
    ws[2 * lanes:] = lo
    rows = lax.broadcasted_iota(jnp.int32, (count + 2 * HALO, lanes), 0) + (me * count - HALO)
    state[moved] = jnp.where((rows >= 0) & (rows < count * peers), 1.0, 0.0)

    up = lax.broadcasted_iota(jnp.int32, (slots, slots), 0)
    across = lax.broadcasted_iota(jnp.int32, (slots, slots), 1)
    tri = ones_where(up <= across)
    blocks = order[...]
    source, slot = lax.div(blocks, slots), lax.rem(blocks, slots)
    mine = source == me
    rank = dot(ones_where(mine), tri) - 1.0
    rank = jnp.where(mine, rank, -1.0)
    tall = lax.broadcasted_iota(jnp.int32, (slots, peers), 0)
    wide = lax.broadcasted_iota(jnp.int32, (slots, peers), 1)
    repeat = ones_where(lax.div(tall, pair) == wide)
    rank_all = dot(repeat, rank.astype(jnp.bfloat16))
    slot_all = dot(repeat, slot.astype(jnp.float32).astype(jnp.bfloat16))
    hit = rank_all == lax.rem(up, pair).astype(jnp.float32)
    send_slot = jnp.sum(jnp.where(hit, slot_all, 0.0), axis=1, keepdims=True)
    sends = jnp.where(send_slot == across.astype(jnp.float32), 1.0, 0.0)
    to_send[...] = sends.astype(jnp.bfloat16)
    from_send[...] = sends.T.astype(jnp.bfloat16)
    own = order[pl.ds(me, 1), :]
    own_source = lax.div(own, slots)
    peer_ids = lax.broadcasted_iota(jnp.int32, (peers, slots), 0)
    from_peer = peer_ids == own_source
    seen = dot(ones_where(from_peer), tri) - 1.0
    own_rank = jnp.sum(jnp.where(from_peer, seen, 0.0), axis=0, keepdims=True)
    place = own_source.astype(jnp.float32) * float(pair) + own_rank
    places = jnp.where(up.astype(jnp.float32) == place, 1.0, 0.0)
    to_place[...] = places.astype(jnp.bfloat16)
    from_place[...] = places.T.astype(jnp.bfloat16)
    here = lax.broadcasted_iota(jnp.int32, (1, peers), 1) == me
    limit = jnp.sum(jnp.where(here, counts[...].astype(jnp.float32), 0.0), axis=1, keepdims=True)
    live[...] = jnp.where(lax.broadcasted_iota(jnp.int32, (1, slots), 1).astype(jnp.float32) < limit, 1.0, 0.0)
    for copy in copies:
        copy.wait()


def end_kernel(peers, traces, observed, to_send, from_send, to_place, from_place,
               residual, misfit, adjoint, sent, got, send_sem, recv_sem):
    width, slots = observed.shape
    lanes = sent.shape[-1]
    wide = traces.shape[0]
    pair = slots // peers
    me = lax.axis_index("mx")
    barrier = greet(peers, me)
    synth = traces[...].T
    packed = permute(to_send[...], synth)
    obs = permute(to_place[...], observed[...].T)
    row = jnp.concatenate([packed, obs, zeros(slots, lanes - wide - width)], axis=1)
    sent[...] = row.reshape(peers, pair, lanes)
    pl.semaphore_wait(barrier, peers - 1)

    def copy_to(off):
        dest = lax.rem(me + off, peers)
        return pltpu.make_async_remote_copy(
            src_ref=sent.at[dest], dst_ref=got.at[me], send_sem=send_sem.at[dest], recv_sem=recv_sem.at[me],
            device_id={"mx": dest}, device_id_type=pl.DeviceIdType.MESH)

    def copy_from(off):
        src = lax.rem(me - off + peers, peers)
        return pltpu.make_async_remote_copy(
            src_ref=sent.at[src], dst_ref=got.at[src], send_sem=send_sem.at[src], recv_sem=recv_sem.at[src],
            device_id={"mx": src}, device_id_type=pl.DeviceIdType.MESH)

    def begin(off, _):
        copy_to(off).start()
        return 0

    def finish(off, _):
        copy_from(off).wait_recv()
        return 0

    def drain(off, _):
        copy_to(off).wait_send()
        return 0

    lax.fori_loop(1, peers, begin, 0)
    got[pl.ds(me, 1)] = sent[pl.ds(me, 1)]
    lax.fori_loop(1, peers, finish, 0)
    arrived = got[...].reshape(slots, lanes)
    placed = permute(from_place[...], arrived[:, :wide]).T
    res = placed[width:width + 1] * (placed[:width] - observed[...])
    residual[...] = res
    misfit[...] = 0.5 * jnp.sum(res * res, axis=0, keepdims=True)
    slot_obs = permute(from_send[...], arrived[:, wide:wide + width]).T
    plain = traces[width:width + 1, :] * (traces[0:width, :] - slot_obs)
    a = lax.broadcasted_iota(jnp.int32, (width, width), 0)
    b = lax.broadcasted_iota(jnp.int32, (width, width), 1)
    back = ones_where((lax.div(a, STEPS) == lax.div(b, STEPS)) & (lax.rem(a, STEPS) + lax.rem(b, STEPS) == STEPS - 1))
    adjoint[...] = permute(back, plain)
    lax.fori_loop(1, peers, drain, 0)


def wave_kernel(state, wb, ws, elem, live, cpl, out, ubuf, lhs, hist):
    fields = ubuf.shape[1]
    lanes = state.shape[2]
    count = state.shape[1] - 2 * HALO
    first = GUARD + HALO
    kdim = wb.shape[0] // 2
    rows_all = ubuf.shape[2]
    metric = state.at[fields:fields + 3]
    mask = state.at[fields + 3]
    for b in range(2):
        for f in range(fields):
            ubuf[b, f, 0:GUARD] = zeros(GUARD, lanes)
            ubuf[b, f, rows_all - GUARD:] = zeros(GUARD, lanes)
            if b:
                ubuf[b, f] = zeros(rows_all, lanes)
            else:
                ubuf[b, f, GUARD:rows_all - GUARD] = state[f] * mask[...]

    def mix(src, c, halo, slab):
        rows = count + 2 * halo
        base = first - halo
        for gi in range(3):
            g = c * 3 + gi
            for r in range(0, rows, slab):
                acc = [None] * 3
                for f in range(fields):
                    uf = ubuf[src, f, base + r:base + r + slab]
                    for k in range(3):
                        term = cpl[(k * fields + g) * fields + f] * uf
                        acc[k] = term if acc[k] is None else acc[k] + term
                at = gi * rows + r
                mid = ubuf[src, g, base + r:base + r + slab]
                vals = [acc[k] * metric[k, HALO - halo + r:HALO - halo + r + slab] for k in range(3)]
                vals.append(ubuf[src, g, base + r - 1:base + r - 1 + slab] - mid)
                vals.append(ubuf[src, g, base + r + 1:base + r + 1 + slab] - mid)
                for k, v in enumerate(vals):
                    hi, lo = split(v)
                    lhs[c, at:at + slab, k * lanes:(k + 1) * lanes] = hi
                    lhs[c, at:at + slab, kdim + k * lanes:kdim + (k + 1) * lanes] = lo

    def apply(src, dst, c, halo):
        rows = count + 2 * halo
        base = first - halo
        res = jnp.dot(lhs[c, :3 * rows], wb[...], preferred_element_type=jnp.float32)
        for gi in range(3):
            g = c * 3 + gi
            part = res[gi * rows:(gi + 1) * rows]
            new = ubuf[src, g, base:base + rows] + (part[:, :lanes] + part[:, lanes:])
            ubuf[dst, g, base:base + rows] = new * mask[HALO - halo:HALO - halo + rows]

    def step(halo, slab, t, _):
        src = lax.rem(t, 2)
        dst = 1 - src
        mix(src, 0, halo, slab)
        mix(src, 1, halo, slab)
        apply(src, dst, 0, halo)
        mix(src, 2, halo, slab)
        apply(src, dst, 1, halo)
        apply(src, dst, 2, halo)
        mine = slice(first, first + count)
        vals = [ubuf[dst, c, mine] for c in range(3)]
        vals.append((ubuf[dst, 3, mine] + ubuf[dst, 4, mine] + ubuf[dst, 5, mine]) / 3.0)
        for c, v in enumerate(vals):
            hi, lo = split(v)
            hist[t, c, :, 0:lanes] = hi
            hist[t, c, :, lanes:2 * lanes] = lo
            hist[t, c, :, 2 * lanes:] = hi
        return 0

    lax.fori_loop(0, 3, functools.partial(step, 16, 80), 0)
    lax.fori_loop(3, STEPS, functools.partial(step, 8, 48), 0)

    slots = ws.shape[1]
    ids = lax.broadcasted_iota(jnp.int32, (count, slots), 0)
    pick = jnp.where(ids == elem[...], live[...], 0.0)

    out[...] = zeros(*out.shape)
    out[COMPS * STEPS:COMPS * STEPS + 1, :] = live[...]

    def sample(t, _):
        for c in range(COMPS):
            prod = jnp.dot(hist[t, c], ws[...], preferred_element_type=jnp.float32)
            out[pl.ds(c * STEPS + t, 1), :] = jnp.sum(prod * pick, axis=0, keepdims=True)
        return 0

    lax.fori_loop(0, STEPS, sample, 0)


VM = pl.BlockSpec(memory_space=pltpu.VMEM)


def shards(initial, derivative, coupling, face_lift, metric, rec_element, rec_weight, live_counts, shot_order, observed):
    fields, nodes, count = initial.shape
    lanes = -(-nodes // 128) * 128
    slots, width = observed.shape
    peers = lax.axis_size("mx")
    span = count + 2 * HALO
    kdim = (derivative.shape[0] + face_lift.shape[0]) * lanes
    wide = -(-(width + 1) // 64) * 64
    f32, bf16 = jnp.float32, jnp.bfloat16
    square = jax.ShapeDtypeStruct((slots, slots), bf16)
    state, wb, ws, to_send, from_send, to_place, from_place, live = pl.pallas_call(
        functools.partial(start_kernel, peers),
        out_shape=(
            jax.ShapeDtypeStruct((fields + metric.shape[0] + 1, span, lanes), f32),
            jax.ShapeDtypeStruct((2 * kdim, 2 * lanes), bf16),
            jax.ShapeDtypeStruct((3 * lanes, slots), bf16),
            square, square, square, square,
            jax.ShapeDtypeStruct((1, slots), f32),
        ),
        in_specs=[VM] * 7,
        out_specs=[VM] * 8,
        scratch_shapes=[
            pltpu.VMEM((lanes, lanes), f32),
            pltpu.VMEM((lanes, slots), f32),
            pltpu.SemaphoreType.DMA((2,)),
            pltpu.SemaphoreType.DMA((2,)),
        ],
        compiler_params=pltpu.CompilerParams(collective_id=0, has_side_effects=True),
        name="start",
    )(initial, metric, derivative, face_lift, rec_weight, shot_order.reshape(peers, slots), live_counts[None, :])
    traces = pl.pallas_call(
        wave_kernel,
        out_shape=jax.ShapeDtypeStruct((wide, slots), f32),
        in_specs=[VM] * 5 + [pl.BlockSpec(memory_space=pltpu.SMEM)],
        out_specs=VM,
        scratch_shapes=[
            pltpu.VMEM((2, fields, span + 2 * GUARD, lanes), f32),
            pltpu.VMEM((3, 3 * span, 2 * kdim), bf16),
            pltpu.VMEM((STEPS, COMPS, count, 3 * lanes), bf16),
        ],
        name="waves",
    )(state, wb, ws, rec_element[None, :], live, coupling.reshape(-1))
    residual, misfit, adjoint = pl.pallas_call(
        functools.partial(end_kernel, peers),
        out_shape=(
            jax.ShapeDtypeStruct((width, slots), f32),
            jax.ShapeDtypeStruct((1, slots), f32),
            jax.ShapeDtypeStruct((width, slots), f32),
        ),
        in_specs=[VM] * 6,
        out_specs=[VM] * 3,
        scratch_shapes=[
            pltpu.VMEM((peers, slots // peers, lanes), f32),
            pltpu.VMEM((peers, slots // peers, lanes), f32),
            pltpu.SemaphoreType.DMA((peers,)),
            pltpu.SemaphoreType.DMA((peers,)),
        ],
        compiler_params=pltpu.CompilerParams(collective_id=1, has_side_effects=True),
        name="finish",
    )(traces, observed.T, to_send, from_send, to_place, from_place)
    return residual.T, misfit[0], adjoint.T


def solution(mesh):
    in_specs = (
        P("shots", None, "mx"),
        P(),
        P(),
        P(),
        P(None, "mx"),
        P("mx"),
        P(None, "mx"),
        P(),
        P(),
        P(("shots", "mx"), None),
    )
    out_specs = (P(("shots", "mx"), None), P(("shots", "mx")), P(("shots", "mx"), None))
    return jax.shard_map(shards, mesh=mesh, in_specs=in_specs, out_specs=out_specs, check_vma=False)
```
